128 devices in a mesh: rep: 2 (over core), dp: 64 (over x, y, z).
Axes of the slice: x: 4, y: 4, z: 4, core: 2. Of those that a mesh axis runs over, the one named last changes fastest.
Arguments:
- x: bfloat16 [128, 2048, 1280], P(('rep', 'dp')), parts along dimension 0
- dy: bfloat16 [128, 2048, 1280], P(('rep', 'dp')), parts along dimension 0
- w_gate: bfloat16 [2, 1280, 3072], replicated
- w_up: bfloat16 [2, 1280, 3072], replicated
- w_down: bfloat16 [2, 3072, 1280], replicated
- m_w_gate: float32 [2, 1280, 3072], P(None, 'dp')
- m_w_up: float32 [2, 1280, 3072], P(None, 'dp')
- m_w_down: float32 [2, 3072, 1280], P(None, 'dp')
- v_w_gate: float32 [2, 1280, 3072], P(None, 'dp')
- v_w_up: float32 [2, 1280, 3072], P(None, 'dp')
- v_w_down: float32 [2, 3072, 1280], P(None, 'dp')
Outputs:
- output 1: bfloat16 [4, 1280, 3072], P('rep'), parts along dimension 0
- output 2: bfloat16 [4, 1280, 3072], P('rep'), parts along dimension 0
- output 3: bfloat16 [4, 3072, 1280], P('rep'), parts along dimension 0
- output 4: float32 [4, 1280, 3072], P('rep', 'dp'), parts along dimension 0
- output 5: float32 [4, 1280, 3072], P('rep', 'dp'), parts along dimension 0
- output 6: float32 [4, 3072, 1280], P('rep', 'dp'), parts along dimension 0
- output 7: float32 [4, 1280, 3072], P('rep', 'dp'), parts along dimension 0
- output 8: float32 [4, 1280, 3072], P('rep', 'dp'), parts along dimension 0
- output 9: float32 [4, 3072, 1280], P('rep', 'dp'), parts along dimension 0
There are 2 independent parts. The reference program is written for one: setup_inputs(seed, part) draws one part's arguments, and reference() takes and returns one part's arrays. A program takes and returns all parts, laid end to end along the dimension named above; an argument that names none is the same for every part.
All inputs are finite; a program needn't handle non-finite values.
Results may differ from the reference program's by a relative error of at most 0.022.
Values are sent between devices in bfloat16 or wider.
A program may use at most 1.5 GiB of HBM per device.

```python
import jax
import jax.numpy as jnp
from jax import lax

SEQUENCES = 64
TOKENS = 2048
D = 1280
FF = 3072
LAYERS = 2
NAMES = ("w_gate", "w_up", "w_down")
SHAPES = {"w_gate": (LAYERS, D, FF), "w_up": (LAYERS, D, FF), "w_down": (LAYERS, FF, D)}


def bump(key, n, height):
    away = (jnp.arange(n, dtype=jnp.int32) - jax.random.randint(key, (), 0, n, jnp.int32)) % n
    return jnp.where(away < n // 8, height, 1.0)


def together(key, own, strength):
    shared = jax.random.normal(key, own.shape[1:], jnp.float32)
    return (own + strength * shared) * lax.rsqrt(1 + strength * strength)


def setup_inputs(seed: int = 0, part: int = 0) -> dict:
    kx, kdy, ka, kb, kz, kf, kh, kl, *keys = jax.random.split(jax.random.key(seed), 8 + 3 * len(NAMES))
    kx, kdy, ka, kb = (jax.random.fold_in(k, part) for k in (kx, kdy, ka, kb))
    kw, km, kv = (keys[i::3] for i in range(3))
    shape = (SEQUENCES, TOKENS, D)
    much_x, much_dy = jax.random.uniform(kz, (2,), jnp.float32, 0.0, 1.0)
    loud = 2.0 ** jax.random.uniform(jax.random.fold_in(kz, 1), (), jnp.float32, -1.0, 2.0)
    layers = 2.0 ** jax.random.uniform(kl, (LAYERS, 1, 1), jnp.float32, -1.0, 1.0)
    x = together(ka, jax.random.normal(kx, shape, jnp.float32), much_x) * bump(kf, D, 4.0)
    dy = together(kb, jax.random.normal(kdy, shape, jnp.float32), much_dy)
    drawn = {"x": x.astype(jnp.bfloat16), "dy": (loud * dy * (SEQUENCES * TOKENS) ** -0.5).astype(jnp.bfloat16)}
    for key, name in zip(kw, NAMES, strict=True):
        w = jax.random.normal(key, SHAPES[name], jnp.float32) * SHAPES[name][1] ** -0.5
        drawn[name] = (w * {"w_gate": 1.0, "w_up": bump(kh, FF, 4.0), "w_down": layers}[name]).astype(jnp.bfloat16)
    for key, name in zip(km, NAMES, strict=True):
        drawn[f"m_{name}"] = 0.1 * jax.random.normal(key, SHAPES[name], jnp.float32)
    for key, name in zip(kv, NAMES, strict=True):
        drawn[f"v_{name}"] = jax.random.uniform(key, SHAPES[name], jnp.float32, 0.005, 0.015)
    return drawn


def matmul(a, w):
    return jnp.dot(a, w, preferred_element_type=jnp.float32).astype(jnp.bfloat16)


def normed(h):
    wide = h.astype(jnp.float32)
    scale = lax.rsqrt(jnp.mean(wide**2, -1, keepdims=True) + 1e-6)
    return (wide * scale).astype(jnp.bfloat16)


def layer(h, w):
    a = normed(h)
    gate = jnp.dot(a, w["w_gate"], preferred_element_type=jnp.float32)
    up = jnp.dot(a, w["w_up"], preferred_element_type=jnp.float32)
    return h + matmul((jax.nn.silu(gate) * up).astype(jnp.bfloat16), w["w_down"])


def adamw(w, m, v, g):
    m = 0.9 * m + 0.1 * g
    v = 0.95 * v + 0.05 * g * g
    step = m * lax.rsqrt(v + 1e-8) + 0.1 * w
    return (w - 0.02 * step).astype(jnp.bfloat16), m, v


def clipped(gradients, sum_of_squares, count):
    factor = jnp.minimum(1.0, 0.5 * lax.rsqrt(sum_of_squares / count + 1e-30))
    return [g * factor for g in gradients]


def stack(weights, h):
    return lax.scan(lambda h, w: (layer(h, w), None), h, weights)[0]


def reference(x, dy, w_gate, w_up, w_down, m_w_gate, m_w_up, m_w_down, v_w_gate, v_w_up, v_w_down):
    weights = dict(zip(NAMES, (w_gate, w_up, w_down), strict=True))

    def take(so_far, sequence):
        h, by_y = sequence
        _, back = jax.vjp(lambda w: stack(w, h), weights)
        return jax.tree.map(lambda total, term: total + term.astype(jnp.float32), so_far, back(by_y)[0]), None

    none_yet = {name: jnp.zeros(w.shape, jnp.float32) for name, w in weights.items()}
    by_weights, _ = lax.scan(take, none_yet, (x, dy))
    gradients = [by_weights[name].astype(jnp.bfloat16).astype(jnp.float32) for name in NAMES]
    gradients = clipped(gradients, sum(jnp.sum(g * g) for g in gradients), sum(g.size for g in gradients))
    new = [
        adamw(w.astype(jnp.float32), m, v, g)
        for w, m, v, g in zip((w_gate, w_up, w_down), (m_w_gate, m_w_up, m_w_down), (v_w_gate, v_w_up, v_w_down), gradients, strict=True)
    ]
    return tuple(one[which] for which in range(3) for one in new)
```

```python
import functools
import math

import jax
import jax.numpy as jnp
from jax import lax
from jax.experimental import pallas as pl
from jax.experimental.pallas import tpu as pltpu
from jax.sharding import PartitionSpec as P

MESH = pl.DeviceIdType.MESH
F32, BF16 = jnp.float32, jnp.bfloat16
AXES = ("x", "y", "z")
ORDER = ((0, 1, 2), (1, 2, 0), (2, 0, 1))
COLOURS = range(3)
NEAR, ALL = (1, 3), (1, 2, 3)
STEPS = 3
VMEM_LIMIT = 67043328
ROWS, PIECE, WIDE = 80, 256, 1024
LOW, HALF = 16, 640
SHARE = 20
DMA = pltpu.SemaphoreType.DMA


def position():
    return tuple(lax.axis_index(axis) for axis in AXES)


def peer(c, axis, delta):
    return {AXES[axis]: (c[axis] + delta) % 4}


def greet(c, deltas):
    barrier = pltpu.get_barrier_semaphore()
    for axis in range(3):
        for delta in deltas[axis]:
            pl.semaphore_signal(barrier, inc=1, device_id=peer(c, axis, delta), device_id_type=MESH)
    pl.semaphore_wait(barrier, sum(len(d) for d in deltas))


def along(c, axis, d, steps):
    return (c[axis] + 4 - steps + d * (2 * steps - 4)) % 4


def lanes(start, size):
    return pl.ds(start if isinstance(start, int) else pl.multiple_of(start, 128), size)


def loop(n, body):
    lax.fori_loop(0, n, lambda j, carry: (body(j), carry)[1], 0)


def whole_or(index):
    return pl.ds(0, 4) if index is None else pl.ds(index, 1)


def lead_of(sel, relative):
    return tuple(pl.ds(0, 1) if relative is not None and not relative[i] else whole_or(s) for i, s in enumerate(sel))


def columns_of(k, z):
    return lanes(WIDE * k + PIECE * z, PIECE)


class Wide:
    @staticmethod
    def shape(free, halves):
        return (*(4 if f else 1 for f in free[:2]), ROWS, (WIDE if free[2] else PIECE) // halves)

    @staticmethod
    def box(k, sel, half, relative=None):
        wide = (WIDE if sel[2] is None else PIECE) // 2
        start = (WIDE * k if relative is None else 0) + half * wide
        if sel[2] is not None and (relative is None or relative[2]):
            start = start + sel[2] * PIECE
        return (*lead_of(sel[:2], relative), pl.ds(0, ROWS), lanes(start, wide))


class Down:
    @staticmethod
    def shape(free, halves):
        return (*(4 if f else 1 for f in free), LOW, 2 * HALF // halves)

    @staticmethod
    def box(k, sel, half, relative=None):
        return (*lead_of(sel, relative), *(() if relative is not None else (k,)), pl.ds(0, LOW), lanes(half * HALF, HALF))


def free_after(k, phases):
    return tuple(axis not in ORDER[k][:phases] for axis in range(3))


def each(lead, body):
    n = math.prod(lead)

    def at(j, carry):
        index = []
        for size in reversed(lead):
            index.append(j % size if size > 1 else 0)
            j = j // size
        body(tuple(reversed(index)))
        return carry

    if n == 1:
        body((0,) * len(lead))
    else:
        lax.fori_loop(0, n, at, 0)


KINDS = (Wide, Wide, Wide, Down)
TURNS = {kind: tuple((s, n) for s in range(1, STEPS + 1) for n, other in enumerate(KINDS) if other is kind) for kind in (Wide, Down)}


def scatter_scratch():
    shapes = []
    for kind in TURNS:
        for k in COLOURS:
            shapes.append(pltpu.VMEM((2, 2, *kind.shape(free_after(k, 1), 2)), BF16))
    for kind in KINDS:
        for k in COLOURS:
            for p in range(3):
                shapes.append(pltpu.VMEM((2, STEPS, *kind.shape(free_after(k, p + 1), 2)), BF16))
            for p in (1, 2):
                shapes.append(pltpu.VMEM((2, *kind.shape(free_after(k, p + 1), 2)), BF16))
            for p in range(2):
                shapes.append(pltpu.VMEM(kind.shape(free_after(k, p + 1), 1), F32))
    return shapes


def scatter_kernel(*refs):
    refs = iter(refs)
    take = lambda n: [next(refs) for _ in range(n)]
    sources, moments = take(len(KINDS)), take(4)
    outs, (spread,) = take(len(KINDS)), take(1)
    stage, held, first, total = {}, {}, {}, {}
    for kind in TURNS:
        for k in COLOURS:
            stage[kind, k] = next(refs)
    for n in range(len(KINDS)):
        for k in COLOURS:
            for p in range(3):
                held[n, k, p] = next(refs)
            for p in (1, 2):
                first[n, k, p] = next(refs)
            for p in range(2):
                total[n, k, p] = next(refs)
    send_sem, recv_sem, stage_sem, send_moment, recv_moment, local_sem = refs
    c = position()
    greet(c, (NEAR, NEAR, ALL))

    def hop(n, k, d, p, s, source=None):
        to = held[n, k, p].at[d, s]
        return pltpu.make_async_remote_copy(
            src_ref=to if source is None else source,
            dst_ref=to,
            send_sem=send_sem.at[n, 2 * k + d, p, s],
            recv_sem=recv_sem.at[n, 2 * k + d, p, s],
            device_id=peer(c, ORDER[k][p], 1 + 2 * d),
            device_id_type=MESH,
        )

    def selected(k, p, target):
        sel = [None] * 3
        for axis in ORDER[k][:p]:
            sel[axis] = c[axis]
        sel[ORDER[k][p]] = target
        return sel

    def term(kind, k, d, turn):
        s, n = TURNS[kind][turn]
        box = kind.box(k, selected(k, 0, along(c, ORDER[k][0], d, s + 1)), d)
        slot = turn % 2
        return pltpu.make_async_copy(sources[n].at[box], stage[kind, k].at[d, slot], stage_sem.at[int(kind is Down), 2 * k + d, slot])

    def own(n, k, d, p, s):
        kind = KINDS[n]
        if p == 0:
            turn = TURNS[kind].index((s, n))
            term(kind, k, d, turn).wait()
            return stage[kind, k].at[d, turn % 2]
        target = along(c, ORDER[k][p], d, s + 1)
        return total[n, k, p - 1].at[kind.box(k, selected(k, p, target), d, free_after(k, p))]

    def step(n, k, d, p, s):
        kind = KINDS[n]
        shape = kind.shape(free_after(k, p + 1), 2)
        lead, wide = shape[:-2], shape[-1]
        if s == 0 and p == 0:
            hop(n, k, d, p, s, sources[n].at[kind.box(k, selected(k, 0, along(c, ORDER[k][0], d, 1)), d)]).start()
            return
        mine = own(n, k, d, p, s)
        if s == 0:
            out = first[n, k, p].at[d]
            each(lead, lambda i: out.__setitem__(i, mine[i].astype(BF16)))
            hop(n, k, d, p, s, out).start()
            return
        hop(n, k, d, p, s - 1).wait_recv()
        come = held[n, k, p].at[d, s - 1]

        def both(i):
            return come[i].astype(F32) + mine[i].astype(F32)

        if s < STEPS:
            each(lead, lambda i: come.__setitem__(i, both(i).astype(BF16)))
            hop(n, k, d, p, s, come).start()
        elif p < 2:
            out = total[n, k, p]
            each(lead, lambda i: out.__setitem__((*i, slice(None), lanes(d * wide, wide)), both(i)))
        elif kind is Wide:
            outs[n][:, lanes(PIECE * k + wide * d, wide)] = both((0, 0)).astype(BF16)
        else:
            outs[n][k, :, lanes(wide * d, wide)] = both((0, 0, 0)).astype(BF16)
        turn = TURNS[kind].index((s, n)) + 2
        if p == 0 and turn < len(TURNS[kind]):
            term(kind, k, d, turn).start()

    def exchange(j, k, delta):
        return pltpu.make_async_remote_copy(
            src_ref=moments[j].at[:, :, columns_of(k, (c[2] + delta + 1) % 4)],
            dst_ref=spread.at[j, :, c[2], :, pl.ds(PIECE * k, PIECE)],
            send_sem=send_moment.at[j, k, delta],
            recv_sem=recv_moment.at[j, k, delta],
            device_id=peer(c, 2, delta + 1),
            device_id_type=MESH,
        )

    def keep(j, k):
        return pltpu.make_async_copy(
            moments[j].at[:, :, columns_of(k, c[2])], spread.at[j, :, c[2], :, pl.ds(PIECE * k, PIECE)], local_sem.at[j, k]
        )

    pieces = [(j, k) for j in range(4) for k in COLOURS]
    for kind in TURNS:
        for k in COLOURS:
            for turn in range(2):
                loop(2, lambda d: term(kind, k, d, turn).start())
    for slot in range(10):
        phase, s = slot // 3, slot % 3
        for n in range(len(KINDS)):
            for p, s_of in ((phase - 1, STEPS), (phase, 0)) if s == 0 else ((phase, s),):
                if 0 <= p < 3:
                    for k in COLOURS:
                        loop(2, lambda d: step(n, k, d, p, s_of))
        if slot == 4:
            for j, k in pieces:
                loop(3, lambda delta: exchange(j, k, delta).start())
                keep(j, k).start()
    for j, k in pieces:
        loop(3, lambda delta: exchange(j, k, delta).wait())
        keep(j, k).wait()
    for n in range(len(KINDS)):
        for k in COLOURS:
            for p in range(3):
                loop(2 * STEPS, lambda i: hop(n, k, i % 2, p, i // 2).wait_send())


ANYWHERE = pl.BlockSpec(memory_space=pl.ANY)
WHOLE = pl.BlockSpec(memory_space=pltpu.VMEM)


def params(number):
    return pltpu.CompilerParams(collective_id=number, has_side_effects=True, vmem_limit_bytes=VMEM_LIMIT)


def scatter(gradients, moments):
    count = len(KINDS)
    steps = (count, 6, 3, STEPS)
    return pl.pallas_call(
        scatter_kernel,
        out_shape=[jax.ShapeDtypeStruct((ROWS, 3 * PIECE) if kind is Wide else (3, LOW, 2 * HALF), BF16) for kind in KINDS]
        + [jax.ShapeDtypeStruct((4, 2, 4, SHARE, 3 * PIECE), F32)],
        in_specs=[ANYWHERE] * (count + 4),
        out_specs=[WHOLE] * count + [ANYWHERE],
        scratch_shapes=scatter_scratch() + [DMA(steps), DMA(steps), DMA((2, 6, 2)), DMA((4, 3, 3)), DMA((4, 3, 3)), DMA((4, 3))],
        compiler_params=params(1),
        cost_estimate=pl.CostEstimate(flops=10**11, bytes_accessed=10**8, transcendentals=0),
        name="scatter",
    )(*gradients, *moments)


def finish_kernel(count, *refs):
    refs = iter(refs)
    take = lambda n: [next(refs) for _ in range(n)]
    g = [take(3), take(3)]
    spread, m_d, v_d = take(3)
    w, outs = take(3), take(3)
    nmv, nm_d, nv_d = take(3)
    news, (g_wide, w_wide, spread_new, sums, mine) = take(3), take(5)
    send_sem, recv_sem, local_sem, send_sum, recv_sum, send_moment, recv_moment, local_moment = refs
    c = position()
    greet(c, (ALL, ALL, ALL))

    part = jnp.zeros((8, 128), F32)
    for layer in range(2):
        for n in range(2):
            for i in range(6):
                span = slice(128 * i, 128 * i + 128)
                block = g[layer][n][:, span].astype(F32)
                g_wide[layer, n, :, span] = block
                part = part + jnp.sum((block * block).reshape(ROWS // 8, 8, 128), axis=0)
        for i in range(10):
            block = g[layer][2][:, :, 128 * i : 128 * i + 128].astype(F32)
            part = part + jnp.sum((block * block).reshape(6, 8, 128), axis=0)
    for axis in range(3):
        mine[axis] = part
        sums[axis, c[axis]] = part
        copies = [
            pltpu.make_async_remote_copy(
                src_ref=mine.at[axis],
                dst_ref=sums.at[axis, c[axis]],
                send_sem=send_sum.at[axis, delta - 1],
                recv_sem=recv_sum.at[axis, delta - 1],
                device_id=peer(c, axis, delta),
                device_id_type=MESH,
            )
            for delta in ALL
        ]
        for copy in copies:
            copy.start()
        for copy in copies:
            copy.wait()
        part = (sums[axis, 0] + sums[axis, 1]) + (sums[axis, 2] + sums[axis, 3])
    square = jnp.sum(jnp.sum(part, axis=0, keepdims=True), axis=1, keepdims=True)
    factor = jnp.minimum(1.0, 0.5 * lax.rsqrt(square / count + 1e-30))

    def adamw(w, m, v, g):
        g = g * factor
        m = 0.9 * m + 0.1 * g
        v = 0.95 * v + 0.05 * g * g
        return w - 0.02 * (m * lax.rsqrt(v + 1e-8) + 0.1 * w), m, v

    for layer in range(2):
        for k in COLOURS:
            span = slice(PIECE * k, PIECE * k + PIECE)
            for n in range(2):
                w_wide[layer, n, :, span] = w[n][layer, :, span].astype(F32)
                for z in range(4):
                    rows = slice(SHARE * z, SHARE * z + SHARE)
                    new, m, v = adamw(
                        w_wide[layer, n, rows, span], spread[n, layer, z, :, span], spread[n + 2, layer, z, :, span], g_wide[layer, n, rows, span]
                    )
                    w_wide[layer, n, rows, span] = new
                    spread_new[n, layer, z, :, span] = m
                    spread_new[n + 2, layer, z, :, span] = v
                news[n][layer, 0, 0, :, span] = w_wide[layer, n, :, span].astype(BF16)
            new, m, v = adamw(w[2][layer, k].astype(F32), m_d[layer, k], v_d[layer, k], g[layer][2][k].astype(F32))
            news[2][layer, 0, 0, 0, k] = new.astype(BF16)
            nm_d[layer, k] = m
            nv_d[layer, k] = v

    kinds = (Wide, Wide, Down)

    def hop(n, k, d, p, s, local=False):
        axis = ORDER[k][2 - p]
        sel = [None] * 3
        for other in ORDER[k][: 2 - p]:
            sel[other] = c[other]
        sel[axis] = along(c, axis, d, s)
        box = outs[n].at[(slice(None), *kinds[n].box(k, sel, d))]
        source = box
        if p == 0 and s == 0:
            if n < 2:
                source = news[n].at[:, :, :, :, lanes(PIECE * k + PIECE // 2 * d, PIECE // 2)]
            else:
                source = news[n].at[:, :, :, :, k, :, lanes(HALF * d, HALF)]
        if local:
            return pltpu.make_async_copy(source, box, local_sem.at[n, 2 * k + d])
        return pltpu.make_async_remote_copy(
            src_ref=source,
            dst_ref=box,
            send_sem=send_sem.at[n, 2 * k + d, p, s],
            recv_sem=recv_sem.at[n, 2 * k + d, p, s],
            device_id=peer(c, axis, 1 + 2 * d),
            device_id_type=MESH,
        )

    def go(n, k, d, p, s):
        if p == 0 and s == 0:
            hop(n, k, d, p, s, local=True).start()
        hop(n, k, d, p, s).start()

    def arrived(n, k, d, p, s):
        hop(n, k, d, p, s).wait_recv()
        if p == 0 and s == 2:
            hop(n, k, d, 0, 0, local=True).wait()

    def exchange(k, delta):
        return pltpu.make_async_remote_copy(
            src_ref=spread_new.at[:, :, (c[2] + delta + 1) % 4, :, pl.ds(PIECE * k, PIECE)],
            dst_ref=nmv.at[:, :, :, columns_of(k, c[2])],
            send_sem=send_moment.at[k, delta],
            recv_sem=recv_moment.at[k, delta],
            device_id=peer(c, 2, delta + 1),
            device_id_type=MESH,
        )

    def keep(k):
        return pltpu.make_async_copy(
            spread_new.at[:, :, c[2], :, pl.ds(PIECE * k, PIECE)], nmv.at[:, :, :, columns_of(k, c[2])], local_moment.at[k]
        )

    for slot in range(10):
        for n in range(3):
            for k in COLOURS:
                if slot > 0:
                    loop(2, lambda d: arrived(n, k, d, (slot - 1) // 3, (slot - 1) % 3))
            for k in COLOURS:
                if slot < 9:
                    loop(2, lambda d: go(n, k, d, slot // 3, slot % 3))
        if slot == 0:
            for k in COLOURS:
                loop(3, lambda delta: exchange(k, delta).start())
                keep(k).start()
    for k in COLOURS:
        loop(3, lambda delta: exchange(k, delta).wait())
        keep(k).wait()
    for n in range(3):
        for k in COLOURS:
            for p in range(3):
                for s in range(STEPS):
                    loop(2, lambda d: hop(n, k, d, p, s).wait_send())


def finish(count, gradients, spread, m_d, v_d, weights):
    steps = (3, 6, 3, STEPS)
    block = (2, 1, 1, ROWS, 3 * PIECE)
    small = jax.ShapeDtypeStruct(m_d.shape, F32)
    return pl.pallas_call(
        functools.partial(finish_kernel, count),
        out_shape=[
            jax.ShapeDtypeStruct((2, 4, 4, ROWS, 3 * WIDE), BF16),
            jax.ShapeDtypeStruct((2, 4, 4, ROWS, 3 * WIDE), BF16),
            jax.ShapeDtypeStruct((2, 4, 4, 4, 3, LOW, 2 * HALF), BF16),
            jax.ShapeDtypeStruct((4, 2, SHARE, 3 * WIDE), F32),
            small,
            small,
        ],
        in_specs=[WHOLE] * 12,
        out_specs=[ANYWHERE] * 4 + [WHOLE] * 2,
        scratch_shapes=[
            pltpu.VMEM(block, BF16),
            pltpu.VMEM(block, BF16),
            pltpu.VMEM((2, 1, 1, 1, 3, LOW, 2 * HALF), BF16),
            pltpu.VMEM((2, 2, ROWS, 3 * PIECE), F32),
            pltpu.VMEM((2, 2, ROWS, 3 * PIECE), F32),
            pltpu.VMEM(spread.shape, F32),
            pltpu.VMEM((3, 4, 8, 128), F32),
            pltpu.VMEM((3, 8, 128), F32),
            DMA(steps),
            DMA(steps),
            DMA(steps[:2]),
            DMA((3, 3)),
            DMA((3, 3)),
            DMA((3, 3)),
            DMA((3, 3)),
            DMA((3,)),
        ],
        compiler_params=params(2),
        cost_estimate=pl.CostEstimate(flops=10**11, bytes_accessed=10**8, transcendentals=0),
        name="finish",
    )(*gradients, spread, m_d, v_d, *weights)


def dot(a, b, dims):
    return lax.dot_general(a, b, (dims, ((), ())), preferred_element_type=F32)


def normed(h):
    wide = h.astype(F32)
    scale = lax.rsqrt(jnp.mean(wide**2, -1, keepdims=True) + 1e-6)
    return (wide * scale).astype(BF16)


def forward(h, w_gate, w_up):
    a, back = jax.vjp(normed, h)
    gate, up = dot(a, w_gate, ((1,), (0,))), dot(a, w_up, ((1,), (0,)))
    return a, back, gate, up, (jax.nn.silu(gate) * up).astype(BF16)


def hidden_gradient(dy, w_down, gate, up):
    by = dot(dy, w_down, ((1,), (1,))).astype(BF16).astype(F32)
    s = jax.nn.sigmoid(gate)
    return (by * up * (s + gate * s * (1 - s))).astype(BF16), (by * gate * s).astype(BF16)


def weight_gradient(a, d):
    return dot(a, d, ((0,), (0,))).astype(BF16)


def over_x(g):
    return lax.psum_scatter(g, AXES[0], scatter_dimension=0, tiled=True)


def over_yz(g):
    return lax.psum_scatter(g, AXES[1:], scatter_dimension=0, tiled=False)


def body(x, dy, w_gate, w_up, w_down, m_gate, m_up, m_down, v_gate, v_up, v_down):
    h, dy = x[0], dy[0]
    c = position()
    first = forward(h, w_gate[0], w_up[0])
    h = h + dot(first[4], w_down[0], ((1,), (0,))).astype(BF16)
    second = forward(h, w_gate[1], w_up[1])

    gradients = []
    for layer, (a, back, gate, up, act) in ((1, second), (0, first)):
        d_down = weight_gradient(act, dy)
        d_gate, d_up = hidden_gradient(dy, w_down[layer], gate, up)
        gradients.append((weight_gradient(a, d_gate), weight_gradient(a, d_up), d_down))
        if layer:
            da = dot(d_gate, w_gate[layer], ((1,), (1,))).astype(BF16) + dot(d_up, w_up[layer], ((1,), (1,))).astype(BF16)
            dy = dy + back(da)[0]

    (gate_1, up_1, down_1), (gate_0, up_0, down_0) = gradients
    down_1 = over_yz(over_x(down_1).reshape(-1, 3, LOW, 2 * HALF))
    gate_1, up_1, gate_0, up_0, down_0 = lax.optimization_barrier((over_x(gate_1), up_1, gate_0, up_0, down_0))
    gate_1 = jnp.moveaxis(gate_1.reshape(4, ROWS, 3, 4, PIECE), 3, 1)
    gate_1 = over_yz(gate_1.reshape(-1, ROWS, 3 * PIECE))

    by_rows = [g.reshape(4, 4, ROWS, 3 * WIDE) for g in (up_1, gate_0, up_0)]
    up_1, gate_0, up_0, down_0, spread = scatter(
        (*by_rows, down_0.reshape(4, 4, 4, 3, LOW, 2 * HALF)), (m_gate, m_up, v_gate, v_up)
    )

    row, rows = 4 * c[0] + c[1], []
    for w in (w_gate, w_up):
        w = lax.dynamic_slice_in_dim(w, ROWS * row, ROWS, axis=1)
        rows.append(jnp.concatenate([lax.dynamic_slice_in_dim(w, WIDE * k + PIECE * c[2], PIECE, axis=2) for k in COLOURS], axis=2))
    by_colour = (2, 3, LOW, 2 * HALF)
    rows.append(lax.dynamic_slice_in_dim(w_down, 3 * LOW * (4 * row + c[2]), 3 * LOW, axis=1).reshape(by_colour))
    count = float(w_gate.size + w_up.size + w_down.size)
    new_gate, new_up, new_down, moments, m_d, v_d = finish(
        count, (gate_0, up_0, down_0, gate_1, up_1, down_1), spread, m_down.reshape(by_colour), v_down.reshape(by_colour), rows
    )
    return (
        new_gate.reshape(w_gate.shape),
        new_up.reshape(w_up.shape),
        new_down.reshape(w_down.shape),
        moments[0],
        moments[1],
        m_d.reshape(m_down.shape),
        moments[2],
        moments[3],
        v_d.reshape(v_down.shape),
    )


def solution(mesh):
    torus = jax.sharding.Mesh(mesh.devices.reshape(2, 4, 4, 4), ("rep", *AXES))
    moment, everywhere = P(None, AXES), ("rep", *AXES)
    return jax.shard_map(
        body,
        mesh=torus,
        in_specs=(P(everywhere),) * 2 + (P(),) * 3 + (moment,) * 6,
        out_specs=(P("rep"),) * 3 + (P("rep", AXES),) * 6,
        check_vma=False,
    )
```

```python
import functools
import math

import jax
import jax.numpy as jnp
from jax import lax
from jax.experimental import pallas as pl
from jax.experimental.pallas import tpu as pltpu
from jax.sharding import PartitionSpec as P

MESH = pl.DeviceIdType.MESH
F32, BF16 = jnp.float32, jnp.bfloat16
AXES = ("x", "y", "z")
ORDER = ((0, 1, 2), (1, 2, 0), (2, 0, 1))
COLOURS = range(3)
NEAR, ALL = (1, 3), (1, 2, 3)
STEPS = 3
VMEM_LIMIT = 67043328
ROWS, PIECE, WIDE = 80, 256, 1024
LOW, HALF = 16, 640
SHARE = 20
DMA = pltpu.SemaphoreType.DMA


def position():
    return tuple(lax.axis_index(axis) for axis in AXES)


def peer(c, axis, delta):
    return {AXES[axis]: (c[axis] + delta) % 4}


def greet(c, deltas):
    barrier = pltpu.get_barrier_semaphore()
    for axis in range(3):
        for delta in deltas[axis]:
            pl.semaphore_signal(barrier, inc=1, device_id=peer(c, axis, delta), device_id_type=MESH)
    pl.semaphore_wait(barrier, sum(len(d) for d in deltas))


def along(c, axis, d, steps):
    return (c[axis] + 4 - steps + d * (2 * steps - 4)) % 4


def lanes(start, size):
    return pl.ds(start if isinstance(start, int) else pl.multiple_of(start, 128), size)


def loop(n, body):
    lax.fori_loop(0, n, lambda j, carry: (body(j), carry)[1], 0)


def whole_or(index):
    return pl.ds(0, 4) if index is None else pl.ds(index, 1)


def lead_of(sel, relative):
    return tuple(pl.ds(0, 1) if relative is not None and not relative[i] else whole_or(s) for i, s in enumerate(sel))


def columns_of(k, z):
    return lanes(WIDE * k + PIECE * z, PIECE)


class Wide:
    @staticmethod
    def shape(free, halves):
        return (*(4 if f else 1 for f in free[:2]), ROWS, (WIDE if free[2] else PIECE) // halves)

    @staticmethod
    def box(k, sel, half, relative=None):
        wide = (WIDE if sel[2] is None else PIECE) // 2
        start = (WIDE * k if relative is None else 0) + half * wide
        if sel[2] is not None and (relative is None or relative[2]):
            start = start + sel[2] * PIECE
        return (*lead_of(sel[:2], relative), pl.ds(0, ROWS), lanes(start, wide))


class Down:
    @staticmethod
    def shape(free, halves):
        return (*(4 if f else 1 for f in free), LOW, 2 * HALF // halves)

    @staticmethod
    def box(k, sel, half, relative=None):
        return (*lead_of(sel, relative), *(() if relative is not None else (k,)), pl.ds(0, LOW), lanes(half * HALF, HALF))


def free_after(k, phases):
    return tuple(axis not in ORDER[k][:phases] for axis in range(3))


def each(lead, body):
    n = math.prod(lead)

    def at(j, carry):
        index = []
        for size in reversed(lead):
            index.append(j % size if size > 1 else 0)
            j = j // size
        body(tuple(reversed(index)))
        return carry

    if n == 1:
        body((0,) * len(lead))
    else:
        lax.fori_loop(0, n, at, 0)


KINDS = (Wide, Wide, Wide, Down)
TURNS = {kind: tuple((s, n) for s in range(1, STEPS + 1) for n, other in enumerate(KINDS) if other is kind) for kind in (Wide, Down)}


def scatter_scratch():
    shapes = []
    for kind in TURNS:
        for k in COLOURS:
            shapes.append(pltpu.VMEM((2, 2, *kind.shape(free_after(k, 1), 2)), BF16))
    for kind in KINDS:
        for k in COLOURS:
            for p in range(3):
                shapes.append(pltpu.VMEM((2, STEPS, *kind.shape(free_after(k, p + 1), 2)), BF16))
            for p in (1, 2):
                shapes.append(pltpu.VMEM((2, *kind.shape(free_after(k, p + 1), 2)), BF16))
            for p in range(2):
                shapes.append(pltpu.VMEM(kind.shape(free_after(k, p + 1), 1), F32))
    return shapes


def scatter_kernel(*refs):
    refs = iter(refs)
    take = lambda n: [next(refs) for _ in range(n)]
    sources, moments = take(len(KINDS)), take(4)
    outs, (spread,) = take(len(KINDS)), take(1)
    stage, held, first, total = {}, {}, {}, {}
    for kind in TURNS:
        for k in COLOURS:
            stage[kind, k] = next(refs)
    for n in range(len(KINDS)):
        for k in COLOURS:
            for p in range(3):
                held[n, k, p] = next(refs)
            for p in (1, 2):
                first[n, k, p] = next(refs)
            for p in range(2):
                total[n, k, p] = next(refs)
    send_sem, recv_sem, stage_sem, send_moment, recv_moment, local_sem = refs
    c = position()
    greet(c, (NEAR, NEAR, ALL))

    def hop(n, k, d, p, s, source=None):
        to = held[n, k, p].at[d, s]
        return pltpu.make_async_remote_copy(
            src_ref=to if source is None else source,
            dst_ref=to,
            send_sem=send_sem.at[n, 2 * k + d, p, s],
            recv_sem=recv_sem.at[n, 2 * k + d, p, s],
            device_id=peer(c, ORDER[k][p], 1 + 2 * d),
            device_id_type=MESH,
        )

    def selected(k, p, target):
        sel = [None] * 3
        for axis in ORDER[k][:p]:
            sel[axis] = c[axis]
        sel[ORDER[k][p]] = target
        return sel

    def term(kind, k, d, turn):
        s, n = TURNS[kind][turn]
        box = kind.box(k, selected(k, 0, along(c, ORDER[k][0], d, s + 1)), d)
        slot = turn % 2
        return pltpu.make_async_copy(sources[n].at[box], stage[kind, k].at[d, slot], stage_sem.at[int(kind is Down), 2 * k + d, slot])

    def own(n, k, d, p, s):
        kind = KINDS[n]
        if p == 0:
            turn = TURNS[kind].index((s, n))
            term(kind, k, d, turn).wait()
            return stage[kind, k].at[d, turn % 2]
        target = along(c, ORDER[k][p], d, s + 1)
        return total[n, k, p - 1].at[kind.box(k, selected(k, p, target), d, free_after(k, p))]

    def step(n, k, d, p, s):
        kind = KINDS[n]
        shape = kind.shape(free_after(k, p + 1), 2)
        lead, wide = shape[:-2], shape[-1]
        if s == 0 and p == 0:
            hop(n, k, d, p, s, sources[n].at[kind.box(k, selected(k, 0, along(c, ORDER[k][0], d, 1)), d)]).start()
            return
        mine = own(n, k, d, p, s)
        if s == 0:
            out = first[n, k, p].at[d]
            each(lead, lambda i: out.__setitem__(i, mine[i].astype(BF16)))
            hop(n, k, d, p, s, out).start()
            return
        hop(n, k, d, p, s - 1).wait_recv()
        come = held[n, k, p].at[d, s - 1]

        def both(i):
            return come[i].astype(F32) + mine[i].astype(F32)

        if s < STEPS:
            each(lead, lambda i: come.__setitem__(i, both(i).astype(BF16)))
            hop(n, k, d, p, s, come).start()
        elif p < 2:
            out = total[n, k, p]
            each(lead, lambda i: out.__setitem__((*i, slice(None), lanes(d * wide, wide)), both(i)))
        elif kind is Wide:
            outs[n][:, lanes(PIECE * k + wide * d, wide)] = both((0, 0)).astype(BF16)
        else:
            outs[n][k, :, lanes(wide * d, wide)] = both((0, 0, 0)).astype(BF16)
        turn = TURNS[kind].index((s, n)) + 2
        if p == 0 and turn < len(TURNS[kind]):
            term(kind, k, d, turn).start()

    def exchange(j, k, delta):
        return pltpu.make_async_remote_copy(
            src_ref=moments[j].at[:, :, columns_of(k, (c[2] + delta + 1) % 4)],
            dst_ref=spread.at[j, :, c[2], :, pl.ds(PIECE * k, PIECE)],
            send_sem=send_moment.at[j, k, delta],
            recv_sem=recv_moment.at[j, k, delta],
            device_id=peer(c, 2, delta + 1),
            device_id_type=MESH,
        )

    def keep(j, k):
        return pltpu.make_async_copy(
            moments[j].at[:, :, columns_of(k, c[2])], spread.at[j, :, c[2], :, pl.ds(PIECE * k, PIECE)], local_sem.at[j, k]
        )

    pieces = [(j, k) for j in range(4) for k in COLOURS]
    for kind in TURNS:
        for k in COLOURS:
            for turn in range(2):
                loop(2, lambda d: term(kind, k, d, turn).start())
    for slot in range(10):
        phase, s = slot // 3, slot % 3
        for n in range(len(KINDS)):
            for p, s_of in ((phase - 1, STEPS), (phase, 0)) if s == 0 else ((phase, s),):
                if 0 <= p < 3:
                    for k in COLOURS:
                        loop(2, lambda d: step(n, k, d, p, s_of))
        if slot == 4:
            for j, k in pieces:
                loop(3, lambda delta: exchange(j, k, delta).start())
                keep(j, k).start()
    for j, k in pieces:
        loop(3, lambda delta: exchange(j, k, delta).wait())
        keep(j, k).wait()
    for n in range(len(KINDS)):
        for k in COLOURS:
            for p in range(3):
                loop(2 * STEPS, lambda i: hop(n, k, i % 2, p, i // 2).wait_send())


ANYWHERE = pl.BlockSpec(memory_space=pl.ANY)
WHOLE = pl.BlockSpec(memory_space=pltpu.VMEM)


def params(number):
    return pltpu.CompilerParams(collective_id=number, has_side_effects=True, vmem_limit_bytes=VMEM_LIMIT)


def scatter(gradients, moments):
    count = len(KINDS)
    steps = (count, 6, 3, STEPS)
    return pl.pallas_call(
        scatter_kernel,
        out_shape=[jax.ShapeDtypeStruct((ROWS, 3 * PIECE) if kind is Wide else (3, LOW, 2 * HALF), BF16) for kind in KINDS]
        + [jax.ShapeDtypeStruct((4, 2, 4, SHARE, 3 * PIECE), F32)],
        in_specs=[ANYWHERE] * (count + 4),
        out_specs=[WHOLE] * count + [ANYWHERE],
        scratch_shapes=scatter_scratch() + [DMA(steps), DMA(steps), DMA((2, 6, 2)), DMA((4, 3, 3)), DMA((4, 3, 3)), DMA((4, 3))],
        compiler_params=params(1),
        cost_estimate=pl.CostEstimate(flops=10**11, bytes_accessed=10**8, transcendentals=0),
        name="scatter",
    )(*gradients, *moments)


def finish_kernel(count, *refs):
    refs = iter(refs)
    take = lambda n: [next(refs) for _ in range(n)]
    g = [take(3), take(3)]
    spread, m_d, v_d = take(3)
    w, outs = take(3), take(3)
    nmv, nm_d, nv_d = take(3)
    news, (g_wide, w_wide, spread_new, sums, mine) = take(3), take(5)
    send_sem, recv_sem, local_sem, send_sum, recv_sum, send_moment, recv_moment, local_moment = refs
    c = position()
    greet(c, (ALL, ALL, ALL))

    part = jnp.zeros((8, 128), F32)
    for layer in range(2):
        for n in range(2):
            for i in range(6):
                span = slice(128 * i, 128 * i + 128)
                block = g[layer][n][:, span].astype(F32)
                g_wide[layer, n, :, span] = block
                part = part + jnp.sum((block * block).reshape(ROWS // 8, 8, 128), axis=0)
        for i in range(10):
            block = g[layer][2][:, :, 128 * i : 128 * i + 128].astype(F32)
            part = part + jnp.sum((block * block).reshape(6, 8, 128), axis=0)
    for axis in range(3):
        mine[axis] = part
        sums[axis, c[axis]] = part
        copies = [
            pltpu.make_async_remote_copy(
                src_ref=mine.at[axis],
                dst_ref=sums.at[axis, c[axis]],
                send_sem=send_sum.at[axis, delta - 1],
                recv_sem=recv_sum.at[axis, delta - 1],
                device_id=peer(c, axis, delta),
                device_id_type=MESH,
            )
            for delta in ALL
        ]
        for copy in copies:
            copy.start()
        for copy in copies:
            copy.wait()
        part = (sums[axis, 0] + sums[axis, 1]) + (sums[axis, 2] + sums[axis, 3])
    square = jnp.sum(jnp.sum(part, axis=0, keepdims=True), axis=1, keepdims=True)
    factor = jnp.minimum(1.0, 0.5 * lax.rsqrt(square / count + 1e-30))

    def adamw(w, m, v, g):
        g = g * factor
        m = 0.9 * m + 0.1 * g
        v = 0.95 * v + 0.05 * g * g
        return w - 0.02 * (m * lax.rsqrt(v + 1e-8) + 0.1 * w), m, v

    for layer in range(2):
        for k in COLOURS:
            span = slice(PIECE * k, PIECE * k + PIECE)
            for n in range(2):
                w_wide[layer, n, :, span] = w[n][layer, :, span].astype(F32)
                for z in range(4):
                    rows = slice(SHARE * z, SHARE * z + SHARE)
                    new, m, v = adamw(
                        w_wide[layer, n, rows, span], spread[n, layer, z, :, span], spread[n + 2, layer, z, :, span], g_wide[layer, n, rows, span]
                    )
                    w_wide[layer, n, rows, span] = new
                    spread_new[n, layer, z, :, span] = m
                    spread_new[n + 2, layer, z, :, span] = v
                news[n][layer, 0, 0, :, span] = w_wide[layer, n, :, span].astype(BF16)
            new, m, v = adamw(w[2][layer, k].astype(F32), m_d[layer, k], v_d[layer, k], g[layer][2][k].astype(F32))
            news[2][layer, 0, 0, 0, k] = new.astype(BF16)
            nm_d[layer, k] = m
            nv_d[layer, k] = v

    kinds = (Wide, Wide, Down)

    def hop(n, k, d, p, s, local=False):
        axis = ORDER[k][2 - p]
        sel = [None] * 3
        for other in ORDER[k][: 2 - p]:
            sel[other] = c[other]
        sel[axis] = along(c, axis, d, s)
        box = outs[n].at[(slice(None), *kinds[n].box(k, sel, d))]
        source = box
        if p == 0 and s == 0:
            if n < 2:
                source = news[n].at[:, :, :, :, lanes(PIECE * k + PIECE // 2 * d, PIECE // 2)]
            else:
                source = news[n].at[:, :, :, :, k, :, lanes(HALF * d, HALF)]
        if local:
            return pltpu.make_async_copy(source, box, local_sem.at[n, 2 * k + d])
        return pltpu.make_async_remote_copy(
            src_ref=source,
            dst_ref=box,
            send_sem=send_sem.at[n, 2 * k + d, p, s],
            recv_sem=recv_sem.at[n, 2 * k + d, p, s],
            device_id=peer(c, axis, 1 + 2 * d),
            device_id_type=MESH,
        )

    def go(n, k, d, p, s):
        if p == 0 and s == 0:
            hop(n, k, d, p, s, local=True).start()
        hop(n, k, d, p, s).start()

    def arrived(n, k, d, p, s):
        hop(n, k, d, p, s).wait_recv()
        if p == 0 and s == 2:
            hop(n, k, d, 0, 0, local=True).wait()

    def exchange(k, delta):
        return pltpu.make_async_remote_copy(
            src_ref=spread_new.at[:, :, (c[2] + delta + 1) % 4, :, pl.ds(PIECE * k, PIECE)],
            dst_ref=nmv.at[:, :, :, columns_of(k, c[2])],
            send_sem=send_moment.at[k, delta],
            recv_sem=recv_moment.at[k, delta],
            device_id=peer(c, 2, delta + 1),
            device_id_type=MESH,
        )

    def keep(k):
        return pltpu.make_async_copy(
            spread_new.at[:, :, c[2], :, pl.ds(PIECE * k, PIECE)], nmv.at[:, :, :, columns_of(k, c[2])], local_moment.at[k]
        )

    for slot in range(10):
        for n in range(3):
            for k in COLOURS:
                if slot > 0:
                    loop(2, lambda d: arrived(n, k, d, (slot - 1) // 3, (slot - 1) % 3))
            for k in COLOURS:
                if slot < 9:
                    loop(2, lambda d: go(n, k, d, slot // 3, slot % 3))
        if slot == 0:
            for k in COLOURS:
                loop(3, lambda delta: exchange(k, delta).start())
                keep(k).start()
    for k in COLOURS:
        loop(3, lambda delta: exchange(k, delta).wait())
        keep(k).wait()
    for n in range(3):
        for k in COLOURS:
            for p in range(3):
                for s in range(STEPS):
                    loop(2, lambda d: hop(n, k, d, p, s).wait_send())


def finish(count, gradients, spread, m_d, v_d, weights):
    steps = (3, 6, 3, STEPS)
    block = (2, 1, 1, ROWS, 3 * PIECE)
    small = jax.ShapeDtypeStruct(m_d.shape, F32)
    return pl.pallas_call(
        functools.partial(finish_kernel, count),
        out_shape=[
            jax.ShapeDtypeStruct((2, 4, 4, ROWS, 3 * WIDE), BF16),
            jax.ShapeDtypeStruct((2, 4, 4, ROWS, 3 * WIDE), BF16),
            jax.ShapeDtypeStruct((2, 4, 4, 4, 3, LOW, 2 * HALF), BF16),
            jax.ShapeDtypeStruct((4, 2, SHARE, 3 * WIDE), F32),
            small,
            small,
        ],
        in_specs=[WHOLE] * 12,
        out_specs=[ANYWHERE] * 4 + [WHOLE] * 2,
        scratch_shapes=[
            pltpu.VMEM(block, BF16),
            pltpu.VMEM(block, BF16),
            pltpu.VMEM((2, 1, 1, 1, 3, LOW, 2 * HALF), BF16),
            pltpu.VMEM((2, 2, ROWS, 3 * PIECE), F32),
            pltpu.VMEM((2, 2, ROWS, 3 * PIECE), F32),
            pltpu.VMEM(spread.shape, F32),
            pltpu.VMEM((3, 4, 8, 128), F32),
            pltpu.VMEM((3, 8, 128), F32),
            DMA(steps),
            DMA(steps),
            DMA(steps[:2]),
            DMA((3, 3)),
            DMA((3, 3)),
            DMA((3, 3)),
            DMA((3, 3)),
            DMA((3,)),
        ],
        compiler_params=params(2),
        cost_estimate=pl.CostEstimate(flops=10**11, bytes_accessed=10**8, transcendentals=0),
        name="finish",
    )(*gradients, spread, m_d, v_d, *weights)


def dot(a, b, dims):
    return lax.dot_general(a, b, (dims, ((), ())), preferred_element_type=F32)


def normed(h):
    wide = h.astype(F32)
    scale = lax.rsqrt(jnp.mean(wide**2, -1, keepdims=True) + 1e-6)
    return (wide * scale).astype(BF16)


def forward(h, w_gate, w_up):
    a, back = jax.vjp(normed, h)
    gate, up = dot(a, w_gate, ((1,), (0,))), dot(a, w_up, ((1,), (0,)))
    return a, back, gate, up, (jax.nn.silu(gate) * up).astype(BF16)


def hidden_gradient(dy, w_down, gate, up):
    by = dot(dy, w_down, ((1,), (1,))).astype(BF16).astype(F32)
    s = jax.nn.sigmoid(gate)
    return (by * up * (s + gate * s * (1 - s))).astype(BF16), (by * gate * s).astype(BF16)


def weight_gradient(a, d):
    return dot(a, d, ((0,), (0,))).astype(BF16)


def over_x(g):
    return lax.psum_scatter(g, AXES[0], scatter_dimension=0, tiled=True)


def over_yz(g):
    return lax.psum_scatter(g, AXES[1:], scatter_dimension=0, tiled=False)


def body(x, dy, w_gate, w_up, w_down, m_gate, m_up, m_down, v_gate, v_up, v_down):
    h, dy = x[0], dy[0]
    c = position()
    first = forward(h, w_gate[0], w_up[0])
    h = h + dot(first[4], w_down[0], ((1,), (0,))).astype(BF16)
    second = forward(h, w_gate[1], w_up[1])

    gradients = []
    for layer, (a, back, gate, up, act) in ((1, second), (0, first)):
        d_down = weight_gradient(act, dy)
        d_gate, d_up = hidden_gradient(dy, w_down[layer], gate, up)
        gradients.append((weight_gradient(a, d_gate), weight_gradient(a, d_up), d_down))
        if layer:
            da = dot(d_gate, w_gate[layer], ((1,), (1,))).astype(BF16) + dot(d_up, w_up[layer], ((1,), (1,))).astype(BF16)
            down_1, dy = lax.optimization_barrier((over_x(d_down), dy + back(da)[0]))
            down_1 = over_yz(down_1.reshape(-1, 3, LOW, 2 * HALF))

    (gate_1, up_1, _), (gate_0, up_0, down_0) = gradients
    gate_1, gate_0, up_0 = lax.optimization_barrier((over_x(gate_1), gate_0, up_0))
    gate_1 = jnp.moveaxis(gate_1.reshape(4, ROWS, 3, 4, PIECE), 3, 1)
    gate_1 = over_yz(gate_1.reshape(-1, ROWS, 3 * PIECE))

    by_rows = [g.reshape(4, 4, ROWS, 3 * WIDE) for g in (up_1, gate_0, up_0)]
    up_1, gate_0, up_0, down_0, spread = scatter(
        (*by_rows, down_0.reshape(4, 4, 4, 3, LOW, 2 * HALF)), (m_gate, m_up, v_gate, v_up)
    )

    row, rows = 4 * c[0] + c[1], []
    for w in (w_gate, w_up):
        w = lax.dynamic_slice_in_dim(w, ROWS * row, ROWS, axis=1)
        rows.append(jnp.concatenate([lax.dynamic_slice_in_dim(w, WIDE * k + PIECE * c[2], PIECE, axis=2) for k in COLOURS], axis=2))
    by_colour = (2, 3, LOW, 2 * HALF)
    rows.append(lax.dynamic_slice_in_dim(w_down, 3 * LOW * (4 * row + c[2]), 3 * LOW, axis=1).reshape(by_colour))
    count = float(w_gate.size + w_up.size + w_down.size)
    new_gate, new_up, new_down, moments, m_d, v_d = finish(
        count, (gate_0, up_0, down_0, gate_1, up_1, down_1), spread, m_down.reshape(by_colour), v_down.reshape(by_colour), rows
    )
    return (
        new_gate.reshape(w_gate.shape),
        new_up.reshape(w_up.shape),
        new_down.reshape(w_down.shape),
        moments[0],
        moments[1],
        m_d.reshape(m_down.shape),
        moments[2],
        moments[3],
        v_d.reshape(v_down.shape),
    )


def solution(mesh):
    torus = jax.sharding.Mesh(mesh.devices.reshape(2, 4, 4, 4), ("rep", *AXES))
    moment, everywhere = P(None, AXES), ("rep", *AXES)
    return jax.shard_map(
        body,
        mesh=torus,
        in_specs=(P(everywhere),) * 2 + (P(),) * 3 + (moment,) * 6,
        out_specs=(P("rep"),) * 3 + (P("rep", AXES),) * 6,
        check_vma=False,
    )
```
